512 devices in a mesh: dp: 16 (over y_lo, x), space: 32 (over z, y_hi, core).
Axes of the slice: x: 4, y: 8 (y_hi: 2, y_lo: 4; y = y_hi * 4 + y_lo), z: 8, core: 2. Of those that a mesh axis runs over, the one named last changes fastest.
Arguments:
- fields: bfloat16 [16, 100, 131072], P('dp', None, 'space'), may hold values from -6 to 6
- cell_index: int32 [1024, 128], P('space'), may hold values from 0 to 6143
- interp_weight: bfloat16 [1024, 16, 128], P('space'), may hold values from 0 to 2, as said below
- w_in: bfloat16 [100, 1024], replicated, may hold values from -0.625 to 0.625
- ln_gain: float32 [1024], replicated, may hold values from 0.5 to 1.5
- w_qkv: bfloat16 [1024, 3072], P('dp'), may hold values from -0.1875 to 0.1875
- w_out: bfloat16 [1024, 1024], P('dp'), may hold values from -3 to 3
Outputs:
- latent: bfloat16 [16, 16384, 1024], P('dp', 'space')
- update: bfloat16 [16, 16384, 1024], P('dp', 'space')
The draws below stay inside these ranges and needn't reach their ends.
Inputs may be any that keep to these rules, and one draw needn't show every extreme that they name: `interp_weight`: in each block the slots from some count on carry zero weight for all its 16 nodes; that count lies between 48 and 128. `cell_index`: indexes a shard's 4096 cells extended by 1024 cells of each neighbouring shard, lower neighbour first.
All inputs are finite; a program needn't handle non-finite values.
Results may differ from the reference program's by a relative error of at most 0.0068.
Values may be sent and summed in bfloat16 or wider, within the bound.
A program may use at most 128 MiB of HBM per device.

```python
import math
import jax
import jax.numpy as jnp
from jax import lax

D = 1024
HEADS = 16
CH = 100
NBLK = 16
SLOTS = 128
NODE_DEV = 512
CELL_DEV = 4096
HEAD_SIZE = 64
HALO_C = 1024
HALO_N = 256
BLK_DEV = 32
SAMPLES = 16
NODES = 16384
CELLS = 131072
BLOCKS = 1024
N_SPACE = 32


def draw_interp_weight(key, part):
    count_key, chosen_key, magnitude_key = jax.random.split(key, 3)
    full_shape = (BLOCKS, NBLK, SLOTS)
    live_count = jax.random.randint(count_key, (BLOCKS, 1, 1), 3 * SLOTS // 8, SLOTS + 1)
    slot_index = lax.broadcasted_iota(jnp.int32, full_shape, 2)
    chosen = jax.random.randint(chosen_key, full_shape, 0, 2)
    kept_mask = (slot_index < live_count) & (chosen == 0)
    magnitude = jax.random.uniform(magnitude_key, full_shape, jnp.float32, 0.0, 1.0)
    return jnp.where(kept_mask, magnitude, 0.0).astype(jnp.float32).astype(jnp.bfloat16)


def plant(array, rng, low, largest):
    spot = [jax.random.randint(jax.random.fold_in(rng, axis), (), 0, length) for axis, length in enumerate(array.shape)]
    longest = array.shape.index(max(array.shape))
    beside = spot[:longest] + [(spot[longest] + 1) % array.shape[longest]] + spot[longest + 1:]
    return array.at[tuple(spot)].set(low).at[tuple(beside)].set(largest)


def block_scale(stream_key, dims, shards, least, top_value):
    level, own = 1.0, jax.random.fold_in(stream_key, 6)
    for axis_at, shards_of in shards:
        heights = jnp.exp(jax.random.uniform(jax.random.fold_in(own, axis_at), (shards_of,), jnp.float32, least / len(shards), top_value / len(shards)))
        level = level * jnp.repeat(heights, dims[axis_at] // shards_of).reshape([-1 if axis == axis_at else 1 for axis in range(len(dims))])
    return level


def bell_draw(key, extent, width, bound, shards=(), kind=jnp.bfloat16):
    entries = width * jax.random.normal(key, extent, jnp.float32)
    if shards:
        entries = entries * block_scale(key, extent, shards, -0.22, 0.18)
    return jnp.clip(entries, -bound, bound).astype(kind)


def setup_inputs(seed: int = 0) -> dict:
    seeds = jax.random.split(jax.random.key(seed), 8)
    fields = bell_draw(seeds[0], (SAMPLES, CH, CELLS), 1.0, 6.0, ((0, 16), (2, 32)))
    cell_index = plant(jax.random.randint(seeds[1], (BLOCKS, SLOTS), 0, CELL_DEV + 2 * HALO_C), jax.random.fold_in(seeds[1], 1), 0, (CELL_DEV + 2 * HALO_C) - 1).astype(jnp.int32)
    interp_weight = draw_interp_weight(jax.random.fold_in(seeds[7], 71), 0)
    w_in = bell_draw(seeds[3], (CH, D), CH ** -0.5, 0.625)
    ln_gain = jnp.clip(1.0 + 0.1 * jax.random.normal(seeds[4], (D,), jnp.float32), 0.5, 1.5)
    w_qkv = bell_draw(seeds[5], (D, 3 * D), D ** -0.5, 0.1875, ((0, 16),))
    w_out = bell_draw(seeds[6], (D, D), (max(D // 256, 1)) ** -0.5, 3.0, ((0, 16),))
    return {"fields": fields, "cell_index": cell_index, "interp_weight": interp_weight, "w_in": w_in, "ln_gain": ln_gain, "w_qkv": w_qkv, "w_out": w_out}


def unit_heads(projected):
    head_rows = projected.reshape(projected.shape[0], HEADS, HEAD_SIZE)
    scale_rows = jnp.sqrt(lax.optimization_barrier(jnp.mean(head_rows * head_rows, axis=-1, keepdims=True)) + 1e-06)
    return (head_rows / scale_rows).astype(jnp.bfloat16)

def one_sample(grid_field, cell_index, interp_weight, w_in, ln_gain, w_qkv, w_out):
    owner_shard = jnp.arange(BLOCKS, dtype=jnp.int32) // BLK_DEV
    source = (owner_shard[:, None] * CELL_DEV - HALO_C + cell_index) % CELLS
    picked = jnp.take(grid_field, source.astype(jnp.int32), axis=1).astype(jnp.float32)
    encoded = jnp.einsum('cbs,bns->bnc', picked, interp_weight.astype(jnp.float32))
    encoded = encoded.reshape(NODES, CH).astype(jnp.bfloat16)
    embedded = jnp.dot(encoded, w_in, preferred_element_type=jnp.float32)
    average = lax.optimization_barrier(jnp.mean(embedded, axis=1, keepdims=True))
    centered = embedded - average
    spread = lax.optimization_barrier(jnp.mean(centered * centered, axis=1, keepdims=True))
    normed = (centered / jnp.sqrt(spread + 1e-05) * ln_gain).astype(jnp.bfloat16)
    projected = jnp.dot(normed, w_qkv, preferred_element_type=jnp.float32)
    queries = unit_heads(projected[:, :D])
    keys_all = unit_heads(projected[:, D:2 * D])
    values_all = projected[:, 2 * D:].reshape(NODES, HEADS, HEAD_SIZE).astype(jnp.bfloat16)
    wrapped_keys = jnp.concatenate([keys_all[NODES - HALO_N:], keys_all, keys_all[:HALO_N]], axis=0)
    wrapped_values = jnp.concatenate([values_all[NODES - HALO_N:], values_all, values_all[:HALO_N]], axis=0)

    def attend(shard_index):
        first_row = shard_index * NODE_DEV
        query_rows = lax.dynamic_slice_in_dim(queries, first_row, NODE_DEV, 0).astype(jnp.float32)
        key_rows = lax.dynamic_slice_in_dim(wrapped_keys, first_row, NODE_DEV + 2 * HALO_N, 0).astype(jnp.float32)
        value_rows = lax.dynamic_slice_in_dim(wrapped_values, first_row, NODE_DEV + 2 * HALO_N, 0).astype(jnp.float32)
        scores = jnp.einsum('qhd,khd->hqk', query_rows, key_rows) / math.sqrt(HEAD_SIZE)
        weights = jnp.exp(scores)
        probs = (weights / lax.optimization_barrier(jnp.sum(weights, axis=2, keepdims=True))).astype(jnp.bfloat16)
        mixed_rows = jnp.einsum('hqk,khd->qhd', probs.astype(jnp.float32), value_rows)
        return mixed_rows.astype(jnp.bfloat16).reshape(NODE_DEV, D)
    attended = lax.map(attend, jnp.arange(N_SPACE, dtype=jnp.int32)).reshape(NODES, D)
    update = jnp.dot(attended, w_out, preferred_element_type=jnp.float32).astype(jnp.bfloat16)
    return (embedded.astype(jnp.bfloat16), update)

def reference(fields, cell_index, interp_weight, w_in, ln_gain, w_qkv, w_out):

    def per_sample(grid_field):
        return one_sample(grid_field, cell_index, interp_weight, w_in, ln_gain, w_qkv, w_out)
    latent, update = lax.map(per_sample, fields)
    return (latent, update)
```

```python
import functools
import math

import jax
import jax.numpy as jnp
from jax import lax
from jax.experimental import pallas as pl
from jax.experimental.pallas import tpu as pltpu
from jax.sharding import PartitionSpec as P

HEADS = 16
CH = 100
HALO_C = 1024
HALO_N = 256
NODE = 512
BLK = 32
CELL = 4096
REACH = CELL + 2 * HALO_C
LANES = 128
MESH = pl.DeviceIdType.MESH
PARTS = (("x", 1), ("x", -1), ("y", 1), ("y", -1))
RELATIVE = (0, -1, 1, 2)
ROWS = 32


def comm_kernel(
    fields, index, weight, w_qkv, w_out,
    enc_out, w_all,
    ext, ext_t, picked, enc, full,
    local_sem, cell_send, cell_recv, enc_send, enc_recv,
    send_sem, recv_sem, pair_send, pair_recv, store_sem,
):
    dp = lax.axis_index("dp")
    sp = lax.axis_index("space")
    x, y = dp % 4, dp // 4
    core, side, z = sp % 2, (sp // 2) % 2, sp // 4

    def at(new_y, new_x, new_side, new_core):
        return (new_y * 4 + new_x, z * 4 + new_side * 2 + new_core)

    up_side = (side + (y + 1) // 4) % 2
    down_side = (side + 1 - (y + 3) // 4) % 2
    step_to = {
        ("x", 1): at(y, (x + 1) % 4, side, core),
        ("x", -1): at(y, (x + 3) % 4, side, core),
        ("y", 1): at((y + 1) % 4, x, up_side, core),
        ("y", -1): at((y + 3) % 4, x, down_side, core),
    }
    partner = at(y, x, side, 1 - core)
    left = (dp, (sp + 31) % 32)
    right = (dp, (sp + 1) % 32)
    far = (dp, (sp + 31 + 2 * core) % 32)

    def rows_of(piece_y, piece_x, half):
        return pl.ds(pl.multiple_of((piece_y * 4 + piece_x) * 64 + half * ROWS, ROWS), ROWS)

    def shard(part):
        if part < 3:
            return w_qkv.at[:, pl.ds(part * 1024, 1024)]
        return w_out

    own_cells = pltpu.make_async_copy(fields, ext.at[:, pl.ds(HALO_C, CELL)], local_sem.at[0])
    own_cells.start()
    own_rows = [
        pltpu.make_async_copy(
            shard(part),
            full.at[part, pl.ds(pl.multiple_of(dp * 64, 64), 64)],
            local_sem.at[1 + part],
        )
        for part in range(4)
    ]
    for copy in own_rows:
        copy.start()

    barrier = pltpu.get_barrier_semaphore()
    for other in list(step_to.values()) + [partner, far]:
        pl.semaphore_signal(barrier, inc=1, device_id=other, device_id_type=MESH)
    pl.semaphore_wait(barrier, 6)

    sent = []

    def remote(src, dst, s_sem, r_sem, target):
        copy = pltpu.make_async_remote_copy(
            src_ref=src, dst_ref=dst, send_sem=s_sem, recv_sem=r_sem,
            device_id=target, device_id_type=MESH,
        )
        copy.start()
        sent.append(copy)
        return copy

    cells_right = remote(
        fields.at[:, pl.ds(CELL - HALO_C, HALO_C)], ext.at[:, pl.ds(0, HALO_C)],
        cell_send.at[0], cell_recv.at[0], right)
    cells_left = remote(
        fields.at[:, pl.ds(0, HALO_C)], ext.at[:, pl.ds(HALO_C + CELL, HALO_C)],
        cell_send.at[1], cell_recv.at[1], left)

    def origin(part, first, second):
        axis = PARTS[part][0]
        if axis == "x":
            return (y + 4 + second) % 4, (x + 4 + first) % 4
        return (y + 4 + first) % 4, (x + 4 + second) % 4

    def slot(first_at, kind):
        return first_at * 3 + kind

    copies = {}

    def move(part, first, second, direction_axis, direction, number):
        piece = origin(part, first, second)
        rows = rows_of(*piece, core)
        if first == 0 and second == 0:
            source = shard(part).at[pl.ds(pl.multiple_of(core * ROWS, ROWS), ROWS)]
        else:
            source = full.at[part, rows]
        copies[part, number] = remote(
            source, full.at[part, rows],
            send_sem.at[part * 15 + number], recv_sem.at[part * 15 + number],
            step_to[direction_axis, direction])

    pairs = {}

    def arrived(part, first, second, number):
        rows = rows_of(*origin(part, first, second), core)
        copies[part, number].wait_recv()
        pairs[part, number] = remote(
            full.at[part, rows], full.at[part, rows],
            pair_send.at[part * 15 + number], pair_recv.at[part * 15 + number], partner)

    def other_axis(part):
        return "y" if PARTS[part][0] == "x" else "x"

    for part, (axis, hand) in enumerate(PARTS):
        move(part, 0, 0, axis, 1, 0)
        move(part, 0, 0, axis, -1, 1)
    for part, (axis, hand) in enumerate(PARTS):
        move(part, 0, 0, other_axis(part), 1, 3 + slot(0, 0))
        move(part, 0, 0, other_axis(part), -1, 3 + slot(0, 1))

    def second_axis_out(part, first_at):
        first = RELATIVE[first_at]
        move(part, first, 0, other_axis(part), 1, 3 + slot(first_at, 0))
        move(part, first, 0, other_axis(part), -1, 3 + slot(first_at, 1))

    def turn(start, count):
        @pl.loop(0, count)
        def _(i):
            at_cell = pl.multiple_of(start + i * LANES, LANES)
            ext_t[pl.ds(at_cell, LANES), 0:CH] = ext[:, pl.ds(at_cell, LANES)].astype(jnp.float32).T

    own_cells.wait()
    turn(HALO_C, CELL // LANES)

    def stage_one():
        for part, (axis, hand) in enumerate(PARTS):
            arrived(part, -1, 0, 0)
            if hand == 1:
                move(part, -1, 0, axis, 1, 2)
            second_axis_out(part, 1)
            arrived(part, 1, 0, 1)
            if hand == -1:
                move(part, 1, 0, axis, -1, 2)
            second_axis_out(part, 2)

    def stage_two():
        for part in range(4):
            arrived(part, 2, 0, 2)
            second_axis_out(part, 3)

    def stage_three(first_at):
        first = RELATIVE[first_at]
        for part, (axis, hand) in enumerate(PARTS):
            arrived(part, first, -1, 3 + slot(first_at, 0))
            if hand == 1:
                move(part, first, -1, other_axis(part), 1, 3 + slot(first_at, 2))
            arrived(part, first, 1, 3 + slot(first_at, 1))
            if hand == -1:
                move(part, first, 1, other_axis(part), -1, 3 + slot(first_at, 2))

    def stage_four(first_at):
        for part in range(4):
            arrived(part, RELATIVE[first_at], 2, 3 + slot(first_at, 2))

    def encode(first_block, count):
        @pl.loop(first_block, first_block + count)
        def _(b):
            @pl.loop(0, LANES // 16)
            def _(group):
                for k in range(16):
                    j = group * 16 + k
                    picked[pl.ds(b * LANES + j, 1), :] = ext_t[pl.ds(index[b, j], 1), :]
        @pl.loop(first_block, first_block + count)
        def _(b):
            rows = picked[pl.ds(pl.multiple_of(b * LANES, LANES), LANES), :].astype(jnp.bfloat16)
            mixed = jnp.dot(weight[b], rows, preferred_element_type=jnp.float32)
            lane = lax.broadcasted_iota(jnp.int32, mixed.shape, 1)
            enc[pl.ds(pl.multiple_of(b * 16, 16), 16), :] = jnp.where(lane < CH, mixed, 0.0).astype(jnp.bfloat16)

    stage_one()
    cells_right.wait_recv()
    cells_left.wait_recv()
    turn(0, HALO_C // LANES)
    turn(HALO_C + CELL, HALO_C // LANES)
    stage_two()
    encode(0, 8)
    stage_three(0)
    encode(8, 8)
    enc_left = remote(
        enc.at[pl.ds(0, HALO_N)], enc.at[pl.ds(NODE + HALO_N, HALO_N)],
        enc_send.at[0], enc_recv.at[0], left)
    stage_three(1)
    encode(16, 8)
    stage_three(2)
    encode(24, 8)
    enc_right = remote(
        enc.at[pl.ds(NODE - HALO_N, HALO_N)], enc.at[pl.ds(NODE, HALO_N)],
        enc_send.at[1], enc_recv.at[1], right)
    stage_three(3)
    for first_at in range(4):
        stage_four(first_at)

    stores = []
    for part in range(4):
        own_rows[part].wait()
        for number in range(15):
            pairs[part, number].wait_recv()
        store = pltpu.make_async_copy(full.at[part], w_all.at[part], store_sem.at[part])
        store.start()
        stores.append(store)
    enc_left.wait_recv()
    enc_right.wait_recv()
    enc_out[...] = enc[...]
    for copy in sent:
        copy.wait_send()
    for store in stores:
        store.wait()


def gather_and_encode(fields, cell_index, interp_weight, w_qkv, w_out):
    vmem = pl.BlockSpec(memory_space=pltpu.VMEM)
    anywhere = pl.BlockSpec(memory_space=pl.ANY)
    dma = pltpu.SemaphoreType.DMA
    return pl.pallas_call(
        comm_kernel,
        out_shape=(
            jax.ShapeDtypeStruct((2 * NODE, LANES), jnp.bfloat16),
            jax.ShapeDtypeStruct((4, 1024, 1024), jnp.bfloat16),
        ),
        in_specs=[anywhere, pl.BlockSpec(memory_space=pltpu.SMEM), vmem, anywhere, anywhere],
        out_specs=(vmem, anywhere),
        scratch_shapes=[
            pltpu.VMEM((CH, REACH), jnp.bfloat16),
            pltpu.VMEM((REACH, LANES), jnp.float32),
            pltpu.VMEM((BLK * LANES, LANES), jnp.float32),
            pltpu.VMEM((2 * NODE, LANES), jnp.bfloat16),
            pltpu.VMEM((4, 1024, 1024), jnp.bfloat16),
            dma((5,)), dma((2,)), dma((2,)), dma((2,)), dma((2,)),
            dma((60,)), dma((60,)), dma((60,)), dma((60,)), dma((4,)),
        ],
        compiler_params=pltpu.CompilerParams(
            collective_id=0, has_side_effects=True, vmem_limit_bytes=40 * 1024 * 1024),
        name="gather_encode",
    )(fields, cell_index, interp_weight, w_qkv, w_out)


def main_kernel(
    enc, w_in, gain, w_all,
    latent, update,
    w_pad, weights, normed, queries, keys, values, attended, load_sem,
):
    f32, bf16 = jnp.float32, jnp.bfloat16
    loads = [
        pltpu.make_async_copy(w_all.at[part], weights.at[part], load_sem.at[part])
        for part in range(4)
    ]
    for load in loads:
        load.start()
    w_pad[...] = jnp.zeros_like(w_pad)
    w_pad[0:CH, :] = w_in[...]

    def embed(chunk, keep):
        rows = pl.ds(pl.multiple_of(chunk * 128, 128), 128)
        embedded = jnp.dot(enc[rows, :], w_pad[...], preferred_element_type=f32)
        if keep:
            latent[rows, :] = embedded.astype(bf16)
        average = jnp.mean(embedded, axis=1, keepdims=True)
        centered = embedded - average
        spread = jnp.mean(centered * centered, axis=1, keepdims=True)
        normed[rows, :] = (centered * lax.rsqrt(spread + 1e-05) * gain[...]).astype(bf16)

    @pl.loop(0, 4)
    def _(chunk):
        embed(chunk, True)

    @pl.loop(4, 8)
    def _(chunk):
        embed(chunk, False)

    wide = 256
    row_head = lax.broadcasted_iota(jnp.int32, (wide, wide), 0) // 64
    col_head = lax.broadcasted_iota(jnp.int32, (wide, wide), 1) // 64
    same_head = jnp.where(row_head == col_head, 1.0, 0.0).astype(bf16)

    def unit(projected, factor):
        squares = projected * projected
        high = squares.astype(bf16)
        low = (squares - high.astype(f32)).astype(bf16)
        total = jnp.dot(high, same_head, preferred_element_type=f32) + jnp.dot(
            low, same_head, preferred_element_type=f32)
        return (projected * (lax.rsqrt(total * (1.0 / 64) + 1e-06) * factor)).astype(bf16)

    for load in loads[:3]:
        load.wait()

    @pl.loop(0, 4)
    def _(group):
        cols = pl.ds(pl.multiple_of(group * wide, wide), wide)
        for chunk in range(4):
            rows = slice(chunk * 256, chunk * 256 + 256)
            some = normed[rows, :]
            if chunk < 2:
                queries[rows, cols] = unit(
                    jnp.dot(some, weights[0, :, cols], preferred_element_type=f32),
                    math.log2(math.e) / 8)
            keys[rows, cols] = unit(
                jnp.dot(some, weights[1, :, cols], preferred_element_type=f32), 1.0)
            values[rows, cols] = jnp.dot(
                some, weights[2, :, cols], preferred_element_type=f32).astype(bf16)

    @pl.loop(0, HEADS // 2)
    def _(pair):
        cols = pl.ds(pl.multiple_of(pair * LANES, LANES), LANES)
        key_pair = keys[:, cols]
        value_pair = values[:, cols]
        value_low = lax.broadcasted_iota(jnp.int32, value_pair.shape, 1) < 64
        ones = jnp.ones_like(value_pair)
        value_one = jnp.where(value_low, value_pair, ones)
        value_two = jnp.where(value_low, ones, value_pair)
        for chunk in range(2):
            rows = slice(chunk * 256, chunk * 256 + 256)
            query_pair = queries[rows, cols]
            query_low = lax.broadcasted_iota(jnp.int32, query_pair.shape, 1) < 64
            none = jnp.zeros_like(query_pair)

            def head(query, value):
                scores = lax.dot_general(
                    query, key_pair, (((1,), (1,)), ((), ())), preferred_element_type=f32)
                return jnp.dot(jnp.exp2(scores).astype(bf16), value, preferred_element_type=f32)

            one = head(jnp.where(query_low, query_pair, none), value_one)
            two = head(jnp.where(query_low, none, query_pair), value_two)
            low = lax.broadcasted_iota(jnp.int32, one.shape, 1) < 64
            top = jnp.where(low, one, two)
            total = pltpu.roll(jnp.where(low, two, one), 64, 1)
            attended[rows, cols] = (top / total).astype(bf16)

    loads[3].wait()

    @pl.loop(0, 2)
    def _(chunk):
        rows = pl.ds(pl.multiple_of(chunk * 256, 256), 256)
        update[rows, :] = jnp.dot(
            attended[rows, :], weights[3], preferred_element_type=f32).astype(bf16)


def attend_all(enc, w_in, gain, w_all):
    vmem = pl.BlockSpec(memory_space=pltpu.VMEM)
    bf16 = jnp.bfloat16
    return pl.pallas_call(
        main_kernel,
        out_shape=(jax.ShapeDtypeStruct((NODE, 1024), bf16),) * 2,
        in_specs=[vmem, vmem, vmem, pl.BlockSpec(memory_space=pl.ANY)],
        out_specs=(vmem, vmem),
        scratch_shapes=[
            pltpu.VMEM((LANES, 1024), bf16),
            pltpu.VMEM((4, 1024, 1024), bf16),
            pltpu.VMEM((2 * NODE, 1024), bf16),
            pltpu.VMEM((NODE, 1024), bf16),
            pltpu.VMEM((2 * NODE, 1024), bf16),
            pltpu.VMEM((2 * NODE, 1024), bf16),
            pltpu.VMEM((NODE, 1024), bf16),
            pltpu.SemaphoreType.DMA((4,)),
        ],
        compiler_params=pltpu.CompilerParams(vmem_limit_bytes=48 * 1024 * 1024),
        name="attend_all",
    )(enc, w_in, gain, w_all)


def shards(fields, cell_index, interp_weight, w_in, ln_gain, w_qkv, w_out):
    enc, w_all = gather_and_encode(fields[0], cell_index, interp_weight, w_qkv, w_out)
    latent, update = attend_all(enc, w_in, ln_gain[None], w_all)
    return (latent[None], update[None])


def solution(mesh):
    placed = (
        P("dp", None, "space"),
        P("space", None),
        P("space", None, None),
        P(),
        P(),
        P("dp", None),
        P("dp", None),
    )
    return jax.shard_map(
        shards,
        mesh=mesh,
        in_specs=placed,
        out_specs=(P("dp", "space", None), P("dp", "space", None)),
        check_vma=False,
    )
```

```python
import math

import jax
import jax.numpy as jnp
from jax import lax
from jax.experimental import pallas as pl
from jax.experimental.pallas import tpu as pltpu
from jax.sharding import PartitionSpec as P

HEADS = 16
CH = 100
HALO_C = 1024
HALO_N = 256
NODE = 512
BLK = 32
CELL = 4096
REACH = CELL + 2 * HALO_C
LANES = 128
SHARD = 64
SLAB = 512
WIDE = 256
MESH = pl.DeviceIdType.MESH
F32, BF16 = jnp.float32, jnp.bfloat16
Q, K, V, O = 0, 1, 2, 3
FIRST = {Q: "x", K: "y", V: "y", O: "x"}
ORDER = (K, Q, V)
RELATIVE = (0, -1, 1, 2)


def everything(
    fields, index_hbm, weight_hbm, w_in_hbm, gain_hbm, w_qkv, w_out,
    latent_hbm, update_hbm,
    index, weight, w_in, gain, ext, ext_t, picked, enc, full,
    w_pad, normed, raw, queries, keys, values, attended, latent, update,
    local_sem, own_sem, cell_send, cell_recv, enc_send, enc_recv,
    plane_send, plane_recv, pair_send, pair_recv,
):
    dp = lax.axis_index("dp")
    sp = lax.axis_index("space")
    x, y = dp % 4, dp // 4
    core, side, z = sp % 2, (sp // 2) % 2, sp // 4

    def at(new_y, new_x, new_z, new_side, new_core):
        return (new_y * 4 + new_x, new_z * 4 + new_side * 2 + new_core)

    up_side = (side + (y + 1) // 4) % 2
    down_side = (side + 1 - (y + 3) // 4) % 2
    step_to = {
        ("x", 1): at(y, (x + 1) % 4, z, side, core),
        ("x", -1): at(y, (x + 3) % 4, z, side, core),
        ("y", 1): at((y + 1) % 4, x, z, up_side, core),
        ("y", -1): at((y + 3) % 4, x, z, down_side, core),
    }
    partner = at(y, x, z, side, 1 - core)
    left = (dp, (sp + 31) % 32)
    right = (dp, (sp + 1) % 32)
    far = (dp, (sp + 31 + 2 * core) % 32)

    own_cells = pltpu.make_async_copy(fields, ext.at[:, pl.ds(HALO_C, CELL)], local_sem.at[0])
    own_cells.start()
    small = [
        pltpu.make_async_copy(source, place, local_sem.at[1 + i])
        for i, (source, place) in enumerate(
            ((index_hbm, index), (weight_hbm, weight), (w_in_hbm, w_in), (gain_hbm, gain)))
    ]
    for copy in small:
        copy.start()

    def shard(part, half):
        if part == O:
            return w_out.at[:, pl.ds(pl.multiple_of(half * SLAB, SLAB), SLAB)]
        return w_qkv.at[:, pl.ds(pl.multiple_of(part * 1024 + half * SLAB, SLAB), SLAB)]

    own_rows = {}
    for part in (K, Q, V, O):
        for half in range(2):
            own_rows[part, half] = pltpu.make_async_copy(
                shard(part, half),
                full.at[2 * part + half, pl.ds(pl.multiple_of(dp * SHARD, SHARD), SHARD)],
                own_sem.at[2 * part + half])
            own_rows[part, half].start()

    barrier = pltpu.get_barrier_semaphore()
    for other in list(step_to.values()) + [partner, far]:
        pl.semaphore_signal(barrier, inc=1, device_id=other, device_id_type=MESH)
    pl.semaphore_wait(barrier, 6)

    sent = []

    def remote(src, dst, s_sem, r_sem, target):
        copy = pltpu.make_async_remote_copy(
            src_ref=src, dst_ref=dst, send_sem=s_sem, recv_sem=r_sem,
            device_id=target, device_id_type=MESH,
        )
        copy.start()
        sent.append(copy)
        return copy

    def place(part, first, second, begin=0, size=SHARD):
        if FIRST[part] == "x":
            piece_y, piece_x = (y + 4 + second) % 4, (x + 4 + first) % 4
        else:
            piece_y, piece_x = (y + 4 + first) % 4, (x + 4 + second) % 4
        start = pl.multiple_of((piece_y * 4 + piece_x) * SHARD + begin, 32)
        return full.at[2 * part + core, pl.ds(start, size)]

    plane, pairs = {}, {}

    def move(part, first, second, axis, direction, number, begin=0, size=SHARD):
        target = place(part, first, second, begin, size)
        source = target
        if first == 0 and second == 0:
            source = shard(part, core)
        plane[part, number] = remote(
            source, target, plane_send.at[part * 20 + number], plane_recv.at[part * 20 + number],
            step_to[axis, direction])

    def second_axis(part):
        return "y" if FIRST[part] == "x" else "x"

    def hand_on(part, first, second, unit):
        here = place(part, first, second)
        number = part * 15 + unit
        pairs[part, unit] = remote(here, here, pair_send.at[number], pair_recv.at[number], partner)

    def outward(part, first_at):
        for kind, direction in ((0, 1), (1, -1)):
            move(part, RELATIVE[first_at], 0, second_axis(part), direction, 4 + 4 * first_at + kind)

    def begin(parts):
        for part in parts:
            move(part, 0, 0, FIRST[part], 1, 0)
            move(part, 0, 0, FIRST[part], -1, 1)
        for part in parts:
            outward(part, 0)

    cells_right = remote(
        fields.at[:, pl.ds(CELL - HALO_C, HALO_C)], ext.at[:, pl.ds(0, HALO_C)],
        cell_send.at[0], cell_recv.at[0], right)
    cells_left = remote(
        fields.at[:, pl.ds(0, HALO_C)], ext.at[:, pl.ds(HALO_C + CELL, HALO_C)],
        cell_send.at[1], cell_recv.at[1], left)
    begin(ORDER)

    def stage_one(part):
        for kind, relative, direction, begin in ((0, -1, 1, 0), (1, 1, -1, 32)):
            plane[part, kind].wait_recv()
            move(part, relative, 0, FIRST[part], direction, 2 + kind, begin, 32)
            outward(part, 1 + kind)
            hand_on(part, relative, 0, kind)

    def stage_two(part):
        plane[part, 2].wait_recv()
        plane[part, 3].wait_recv()
        outward(part, 3)
        hand_on(part, 2, 0, 2)

    def stage_three(part, first_at):
        for kind, relative, direction, begin in ((0, -1, 1, 0), (1, 1, -1, 32)):
            number = 4 + 4 * first_at
            plane[part, number + kind].wait_recv()
            move(part, RELATIVE[first_at], relative, second_axis(part), direction,
                 number + 2 + kind, begin, 32)
            hand_on(part, RELATIVE[first_at], relative, 3 + 3 * first_at + kind)

    def stage_four(part, first_at):
        number = 4 + 4 * first_at
        plane[part, number + 2].wait_recv()
        plane[part, number + 3].wait_recv()
        hand_on(part, RELATIVE[first_at], 2, 3 + 3 * first_at + 2)

    def finish(part):
        for half in range(2):
            own_rows[part, half].wait()
        for unit in range(15):
            pairs[part, unit].wait_recv()

    def turn(start, count):
        @pl.loop(0, count // 4)
        def _(i):
            for k in range(4):
                at_cell = pl.multiple_of(start + i * (4 * LANES) + k * LANES, LANES)
                ext_t[pl.ds(at_cell, LANES), 0:CH] = ext[:, pl.ds(at_cell, LANES)].astype(F32).T

    def encode(first_block, count):
        @pl.loop(first_block, first_block + count)
        def _(b):
            base = pl.multiple_of(b * LANES, LANES)
            for j in range(LANES):
                picked[pl.ds(base + j, 1), :] = ext_t[pl.ds(index[b, j], 1), :]
        for b in range(first_block, first_block + count):
            rows = picked[b * LANES:(b + 1) * LANES, :].astype(BF16)
            mixed = jnp.dot(weight[b], rows, preferred_element_type=F32)
            lane = lax.broadcasted_iota(jnp.int32, mixed.shape, 1)
            enc[b * 16:(b + 1) * 16, :] = jnp.where(lane < CH, mixed, 0.0).astype(BF16)

    def embed(chunk, keep):
        rows = slice(chunk * 128, chunk * 128 + 128)
        embedded = jnp.dot(enc[rows, :], w_pad[...], preferred_element_type=F32)
        if keep:
            latent[rows, :] = embedded.astype(BF16)
        average = jnp.mean(embedded, axis=1, keepdims=True)
        centered = embedded - average
        spread = jnp.mean(centered * centered, axis=1, keepdims=True)
        normed[rows, :] = (centered * lax.rsqrt(spread + 1e-05) * gain[...]).astype(BF16)

    row_head = lax.broadcasted_iota(jnp.int32, (WIDE, WIDE), 0) // 64
    col_head = lax.broadcasted_iota(jnp.int32, (WIDE, WIDE), 1) // 64
    same_head = jnp.where(row_head == col_head, 1.0, 0.0).astype(BF16)

    def unit_rows(projected, factor):
        squares = (projected * projected).astype(BF16)
        total = jnp.dot(squares, same_head, preferred_element_type=F32)
        return (projected * (lax.rsqrt(total * (1.0 / 64) + 1e-06) * factor)).astype(BF16)

    def project(part):
        @pl.loop(0, 4)
        def _(group):
            cols = pl.ds(pl.multiple_of(group * WIDE, WIDE), WIDE)
            block = full[2 * part + group // 2, :, pl.ds(pl.multiple_of((group % 2) * WIDE, WIDE), WIDE)]
            for chunk in range(2 if part == Q else 4):
                rows = slice(chunk * 256, chunk * 256 + 256)
                projected = jnp.dot(normed[rows, :], block, preferred_element_type=F32)
                if part == V:
                    values[rows, cols] = projected.astype(BF16)
                else:
                    raw[rows, cols] = projected
        if part == V:
            return

        @pl.loop(0, 4)
        def _(group):
            cols = pl.ds(pl.multiple_of(group * WIDE, WIDE), WIDE)
            for chunk in range(2 if part == Q else 4):
                rows = slice(chunk * 256, chunk * 256 + 256)
                if part == Q:
                    queries[rows, cols] = unit_rows(raw[rows, cols], math.log2(math.e) / 8)
                else:
                    keys[rows, cols] = unit_rows(raw[rows, cols], 1.0)

    own_cells.wait()
    for copy in small:
        copy.wait()
    w_pad[...] = jnp.zeros_like(w_pad)
    w_pad[0:CH, :] = w_in[...]
    turn(HALO_C, CELL // LANES)
    stage_one(Q)
    cells_right.wait_recv()
    turn(0, HALO_C // LANES)
    cells_left.wait_recv()
    turn(HALO_C + CELL, HALO_C // LANES)
    encode(0, 8)
    stage_two(Q)
    encode(8, 8)
    enc_left = remote(
        enc.at[pl.ds(0, HALO_N)], enc.at[pl.ds(NODE + HALO_N, HALO_N)],
        enc_send.at[0], enc_recv.at[0], left)
    stage_one(K)
    encode(16, 8)
    stage_one(V)
    encode(24, 8)
    enc_right = remote(
        enc.at[pl.ds(NODE - HALO_N, HALO_N)], enc.at[pl.ds(NODE, HALO_N)],
        enc_send.at[1], enc_recv.at[1], right)
    embed(0, True)
    embed(1, True)
    stage_two(K)
    embed(2, True)
    stage_two(V)
    embed(3, True)
    latent_out = pltpu.make_async_copy(latent, latent_hbm, local_sem.at[5])
    latent_out.start()
    for quarter in range(4):
        for part in ORDER:
            stage_three(part, quarter)
    enc_left.wait_recv()
    enc_right.wait_recv()
    for quarter in range(4):
        embed(4 + quarter, False)
        for part in ORDER:
            stage_four(part, quarter)
    begin((O,))
    finish(K)
    project(K)
    stage_one(O)
    finish(Q)
    project(Q)
    stage_two(O)
    finish(V)
    project(V)
    for quarter in range(4):
        stage_three(O, quarter)

    def attend(pair):
        cols = pl.ds(pl.multiple_of(pair * LANES, LANES), LANES)
        key_pair = keys[:, cols]
        value_pair = values[:, cols]
        value_low = lax.broadcasted_iota(jnp.int32, value_pair.shape, 1) < 64
        ones = jnp.ones_like(value_pair)
        value_one = jnp.where(value_low, value_pair, ones)
        value_two = jnp.where(value_low, ones, value_pair)
        for chunk in range(2):
            rows = slice(chunk * 256, chunk * 256 + 256)
            query_pair = queries[rows, cols]
            query_low = lax.broadcasted_iota(jnp.int32, query_pair.shape, 1) < 64
            none = jnp.zeros_like(query_pair)

            def head(query, value):
                scores = lax.dot_general(
                    query, key_pair, (((1,), (1,)), ((), ())), preferred_element_type=F32)
                return jnp.dot(jnp.exp2(scores).astype(BF16), value, preferred_element_type=F32)

            one = head(jnp.where(query_low, query_pair, none), value_one)
            two = head(jnp.where(query_low, none, query_pair), value_two)
            low = lax.broadcasted_iota(jnp.int32, one.shape, 1) < 64
            top = jnp.where(low, one, two)
            total = pltpu.roll(jnp.where(low, two, one), 64, 1)
            attended[rows, cols] = (top / total).astype(BF16)

    @pl.loop(0, HEADS // 4)
    def _(pair):
        attend(pair)

    for quarter in range(4):
        stage_four(O, quarter)

    @pl.loop(HEADS // 4, HEADS // 2)
    def _(pair):
        attend(pair)

    finish(O)
    outs = []
    for chunk in range(2):
        rows = slice(chunk * 256, chunk * 256 + 256)
        for half in range(2):
            update[rows, half * SLAB:(half + 1) * SLAB] = jnp.dot(
                attended[rows, :], full[2 * O + half], preferred_element_type=F32).astype(BF16)
        out = pltpu.make_async_copy(
            update.at[pl.ds(chunk * 256, 256)], update_hbm.at[pl.ds(chunk * 256, 256)],
            local_sem.at[6 + chunk])
        out.start()
        outs.append(out)
    for copy in sent:
        copy.wait_send()
    latent_out.wait()
    for out in outs:
        out.wait()


def shards(fields, cell_index, interp_weight, w_in, ln_gain, w_qkv, w_out):
    hbm = pl.BlockSpec(memory_space=pltpu.MemorySpace.HBM)
    dma = pltpu.SemaphoreType.DMA
    vmem = pltpu.VMEM
    latent, update = pl.pallas_call(
        everything,
        out_shape=(jax.ShapeDtypeStruct((NODE, 1024), BF16),) * 2,
        in_specs=[hbm] * 7,
        out_specs=(hbm, hbm),
        scratch_shapes=[
            pltpu.SMEM((BLK, LANES), jnp.int32),
            vmem((BLK, 16, LANES), BF16),
            vmem((CH, 1024), BF16),
            vmem((1, 1024), F32),
            vmem((CH, REACH), BF16),
            vmem((REACH, LANES), F32),
            vmem((BLK * LANES, LANES), F32),
            vmem((2 * NODE, LANES), BF16),
            vmem((8, 1024, SLAB), BF16),
            vmem((LANES, 1024), BF16),
            vmem((2 * NODE, 1024), BF16),
            vmem((2 * NODE, 1024), F32),
            vmem((NODE, 1024), BF16),
            vmem((2 * NODE, 1024), BF16),
            vmem((2 * NODE, 1024), BF16),
            vmem((NODE, 1024), BF16),
            vmem((NODE, 1024), BF16),
            vmem((NODE, 1024), BF16),
            dma((8,)), dma((8,)), dma((2,)), dma((2,)), dma((2,)), dma((2,)),
            dma((80,)), dma((80,)), dma((60,)), dma((60,)),
        ],
        compiler_params=pltpu.CompilerParams(
            collective_id=0, has_side_effects=True, vmem_limit_bytes=60 * 1024 * 1024),
        name="everything",
    )(fields[0], cell_index, interp_weight, w_in, ln_gain[None], w_qkv, w_out)
    return (latent[None], update[None])


def solution(mesh):
    placed = (
        P("dp", None, "space"),
        P("space", None),
        P("space", None, None),
        P(),
        P(),
        P("dp", None),
        P("dp", None),
    )
    return jax.shard_map(
        shards,
        mesh=mesh,
        in_specs=placed,
        out_specs=(P("dp", "space", None), P("dp", "space", None)),
        check_vma=False,
    )
```

```python
import math

import jax
import jax.numpy as jnp
from jax import lax
from jax.experimental import pallas as pl
from jax.experimental.pallas import tpu as pltpu
from jax.sharding import PartitionSpec as P

HEADS = 16
CH = 100
HALO_C = 1024
HALO_N = 256
NODE = 512
BLK = 32
CELL = 4096
REACH = CELL + 2 * HALO_C
LANES = 128
SHARD = 64
SLAB = 512
WIDE = 256
MESH = pl.DeviceIdType.MESH
F32, BF16 = jnp.float32, jnp.bfloat16
Q, K, V, O = 0, 1, 2, 3
FIRST = {Q: "x", K: "y", V: "y", O: "y"}
ORDER = (K, Q, V)
RELATIVE = (0, -1, 1, 2)


def everything(
    fields, index_hbm, weight_hbm, w_in_hbm, gain_hbm, w_qkv, w_out,
    latent, update,
    index, weight, w_in, gain, ext, ext_t, picked, enc, full,
    w_pad, normed, raw, queries, keys, values, attended,
    local_sem, own_sem, cell_send, cell_recv, enc_send, enc_recv,
    plane_send, plane_recv, pair_send, pair_recv,
):
    dp = lax.axis_index("dp")
    sp = lax.axis_index("space")
    x, y = dp % 4, dp // 4
    core, side, z = sp % 2, (sp // 2) % 2, sp // 4

    def at(new_y, new_x, new_z, new_side, new_core):
        return (new_y * 4 + new_x, new_z * 4 + new_side * 2 + new_core)

    up_side = (side + (y + 1) // 4) % 2
    down_side = (side + 1 - (y + 3) // 4) % 2
    step_to = {
        ("x", 1): at(y, (x + 1) % 4, z, side, core),
        ("x", -1): at(y, (x + 3) % 4, z, side, core),
        ("y", 1): at((y + 1) % 4, x, z, up_side, core),
        ("y", -1): at((y + 3) % 4, x, z, down_side, core),
    }
    partner = at(y, x, z, side, 1 - core)
    left = (dp, (sp + 31) % 32)
    right = (dp, (sp + 1) % 32)
    far = (dp, (sp + 31 + 2 * core) % 32)

    own_cells = pltpu.make_async_copy(fields, ext.at[:, pl.ds(HALO_C, CELL)], local_sem.at[0])
    own_cells.start()
    small = [
        pltpu.make_async_copy(source, place, local_sem.at[1 + i])
        for i, (source, place) in enumerate(
            ((index_hbm, index), (weight_hbm, weight), (w_in_hbm, w_in), (gain_hbm, gain)))
    ]
    for copy in small:
        copy.start()

    def shard(part, half):
        if part == O:
            return w_out.at[:, pl.ds(pl.multiple_of(half * SLAB, SLAB), SLAB)]
        return w_qkv.at[:, pl.ds(pl.multiple_of(part * 1024 + half * SLAB, SLAB), SLAB)]

    own_rows = {}
    for part in (K, Q, V, O):
        for half in range(2):
            own_rows[part, half] = pltpu.make_async_copy(
                shard(part, half),
                full.at[2 * part + half, pl.ds(pl.multiple_of(dp * SHARD, SHARD), SHARD)],
                own_sem.at[2 * part + half])
            own_rows[part, half].start()

    barrier = pltpu.get_barrier_semaphore()
    for other in list(step_to.values()) + [partner, far]:
        pl.semaphore_signal(barrier, inc=1, device_id=other, device_id_type=MESH)
    pl.semaphore_wait(barrier, 6)

    sent = []

    def remote(src, dst, s_sem, r_sem, target, grouped=False):
        copy = pltpu.make_async_remote_copy(
            src_ref=src, dst_ref=dst, send_sem=s_sem, recv_sem=r_sem,
            device_id=target, device_id_type=MESH,
        )
        copy.start()
        if not grouped:
            sent.append(copy)
        return copy

    def place(part, first, second, begin=0, size=SHARD):
        if FIRST[part] == "x":
            piece_y, piece_x = (y + 4 + second) % 4, (x + 4 + first) % 4
        else:
            piece_y, piece_x = (y + 4 + first) % 4, (x + 4 + second) % 4
        start = pl.multiple_of((piece_y * 4 + piece_x) * SHARD + begin, 32)
        return full.at[2 * part + core, pl.ds(start, size)]

    plane = {}

    def move(part, first, second, axis, direction, number, begin=0, size=SHARD):
        target = place(part, first, second, begin, size)
        source = target
        if first == 0 and second == 0:
            source = shard(part, core)
        plane[part, number] = remote(
            source, target, plane_send.at[part], plane_recv.at[part * 20 + number],
            step_to[axis, direction], grouped=True)

    def second_axis(part):
        return "y" if FIRST[part] == "x" else "x"

    def hand_on(part, first, second, unit):
        here = place(part, first, second)
        remote(here, here, pair_send.at[part], pair_recv.at[part], partner, grouped=True)

    def all_pieces(part, sem):
        rows = full.at[2 * part, pl.ds(0, 15 * SHARD)]
        pltpu.make_async_copy(rows, rows, sem.at[part]).wait()

    def outward(part, first_at):
        for kind, direction in ((0, 1), (1, -1)):
            move(part, RELATIVE[first_at], 0, second_axis(part), direction, 4 + 4 * first_at + kind)

    def begin(parts):
        for part in parts:
            move(part, 0, 0, FIRST[part], 1, 0)
            move(part, 0, 0, FIRST[part], -1, 1)
        for part in parts:
            outward(part, 0)

    for part in (K, V, Q):
        move(part, 0, 0, FIRST[part], 1, 0)
        move(part, 0, 0, FIRST[part], -1, 1)
    cells_right = remote(
        fields.at[:, pl.ds(CELL - HALO_C, HALO_C)], ext.at[:, pl.ds(0, HALO_C)],
        cell_send.at[0], cell_recv.at[0], right)
    cells_left = remote(
        fields.at[:, pl.ds(0, HALO_C)], ext.at[:, pl.ds(HALO_C + CELL, HALO_C)],
        cell_send.at[1], cell_recv.at[1], left)
    for part in (K, V, Q):
        outward(part, 0)

    def stage_one(part):
        for kind, relative, direction, begin in ((0, -1, 1, 0), (1, 1, -1, 32)):
            plane[part, kind].wait_recv()
            move(part, relative, 0, FIRST[part], direction, 2 + kind, begin, 32)
            outward(part, 1 + kind)
            hand_on(part, relative, 0, kind)

    def stage_two(part):
        plane[part, 2].wait_recv()
        plane[part, 3].wait_recv()
        outward(part, 3)
        hand_on(part, 2, 0, 2)

    def stage_three(part, first_at):
        for kind, relative, direction, begin in ((0, -1, 1, 0), (1, 1, -1, 32)):
            number = 4 + 4 * first_at
            plane[part, number + kind].wait_recv()
            move(part, RELATIVE[first_at], relative, second_axis(part), direction,
                 number + 2 + kind, begin, 32)
            hand_on(part, RELATIVE[first_at], relative, 3 + 3 * first_at + kind)

    def stage_four(part, first_at):
        number = 4 + 4 * first_at
        plane[part, number + 2].wait_recv()
        plane[part, number + 3].wait_recv()
        hand_on(part, RELATIVE[first_at], 2, 3 + 3 * first_at + 2)

    def finish(part):
        for half in range(2):
            own_rows[part, half].wait()
        all_pieces(part, pair_recv)

    def turn(start, count):
        @pl.loop(0, count // 4)
        def _(i):
            for k in range(4):
                at_cell = pl.multiple_of(start + i * (4 * LANES) + k * LANES, LANES)
                ext_t[pl.ds(at_cell, LANES), 0:CH] = ext[:, pl.ds(at_cell, LANES)].astype(F32).T

    def encode(first_block, count):
        @pl.loop(first_block, first_block + count)
        def _(b):
            base = pl.multiple_of(b * LANES, LANES)
            for j in range(LANES):
                picked[pl.ds(base + j, 1), :] = ext_t[pl.ds(index[b, j], 1), :]
        for b in range(first_block, first_block + count):
            rows = picked[b * LANES:(b + 1) * LANES, :].astype(BF16)
            mixed = jnp.dot(weight[b], rows, preferred_element_type=F32)
            lane = lax.broadcasted_iota(jnp.int32, mixed.shape, 1)
            enc[b * 16:(b + 1) * 16, :] = jnp.where(lane < CH, mixed, 0.0).astype(BF16)

    def embed(chunk, keep):
        rows = slice(chunk * 128, chunk * 128 + 128)
        embedded = jnp.dot(enc[rows, :], w_pad[...], preferred_element_type=F32)
        if keep:
            latent[rows, :] = embedded.astype(BF16)
        average = jnp.mean(embedded, axis=1, keepdims=True)
        centered = embedded - average
        spread = jnp.mean(centered * centered, axis=1, keepdims=True)
        normed[rows, :] = (centered * lax.rsqrt(spread + 1e-05) * gain[...]).astype(BF16)

    row_head = lax.broadcasted_iota(jnp.int32, (WIDE, WIDE), 0) // 64
    col_head = lax.broadcasted_iota(jnp.int32, (WIDE, WIDE), 1) // 64
    same_head = jnp.where(row_head == col_head, 1.0, 0.0).astype(BF16)

    def unit_rows(projected, factor):
        squares = (projected * projected).astype(BF16)
        total = jnp.dot(squares, same_head, preferred_element_type=F32)
        return (projected * (lax.rsqrt(total * (1.0 / 64) + 1e-06) * factor)).astype(BF16)

    def project(part):
        @pl.loop(0, 4)
        def _(group):
            cols = pl.ds(pl.multiple_of(group * WIDE, WIDE), WIDE)
            block = full[2 * part + group // 2, :, pl.ds(pl.multiple_of((group % 2) * WIDE, WIDE), WIDE)]
            for chunk in range(2 if part == Q else 4):
                rows = slice(chunk * 256, chunk * 256 + 256)
                projected = jnp.dot(normed[rows, :], block, preferred_element_type=F32)
                if part == V:
                    values[rows, cols] = projected.astype(BF16)
                else:
                    raw[rows, cols] = projected
        if part == V:
            return

        @pl.loop(0, 4)
        def _(group):
            cols = pl.ds(pl.multiple_of(group * WIDE, WIDE), WIDE)
            for chunk in range(2 if part == Q else 4):
                rows = slice(chunk * 256, chunk * 256 + 256)
                if part == Q:
                    queries[rows, cols] = unit_rows(raw[rows, cols], math.log2(math.e) / 8)
                else:
                    keys[rows, cols] = unit_rows(raw[rows, cols], 1.0)

    own_cells.wait()
    for copy in small:
        copy.wait()
    w_pad[...] = jnp.zeros_like(w_pad)
    w_pad[0:CH, :] = w_in[...]
    turn(HALO_C, CELL // LANES)
    stage_one(K)
    stage_one(V)
    stage_one(Q)
    cells_right.wait_recv()
    turn(0, HALO_C // LANES)
    cells_left.wait_recv()
    turn(HALO_C + CELL, HALO_C // LANES)
    encode(0, 8)
    stage_two(K)
    encode(8, 8)
    enc_left = remote(
        enc.at[pl.ds(0, HALO_N)], enc.at[pl.ds(NODE + HALO_N, HALO_N)],
        enc_send.at[0], enc_recv.at[0], left)
    stage_two(V)
    encode(16, 8)
    stage_two(Q)
    encode(24, 8)
    enc_right = remote(
        enc.at[pl.ds(NODE - HALO_N, HALO_N)], enc.at[pl.ds(NODE, HALO_N)],
        enc_send.at[1], enc_recv.at[1], right)
    for quarter in range(4):
        embed(quarter, True)
        for part in ORDER:
            stage_three(part, quarter)
    enc_left.wait_recv()
    enc_right.wait_recv()
    for quarter in range(4):
        stage_four(K, quarter)
    for quarter in range(4):
        embed(4 + quarter, False)
        stage_four(Q, quarter)
        stage_four(V, quarter)
    begin((O,))
    finish(K)
    project(K)
    stage_one(O)
    finish(Q)
    project(Q)
    stage_two(O)
    finish(V)
    project(V)
    for quarter in range(4):
        stage_three(O, quarter)

    def attend(pair):
        cols = pl.ds(pl.multiple_of(pair * LANES, LANES), LANES)
        key_pair = keys[:, cols]
        value_pair = values[:, cols]
        value_low = lax.broadcasted_iota(jnp.int32, value_pair.shape, 1) < 64
        ones = jnp.ones_like(value_pair)
        value_one = jnp.where(value_low, value_pair, ones)
        value_two = jnp.where(value_low, ones, value_pair)
        for chunk in range(2):
            rows = slice(chunk * 256, chunk * 256 + 256)
            query_pair = queries[rows, cols]
            query_low = lax.broadcasted_iota(jnp.int32, query_pair.shape, 1) < 64
            none = jnp.zeros_like(query_pair)

            def head(query, value):
                scores = lax.dot_general(
                    query, key_pair, (((1,), (1,)), ((), ())), preferred_element_type=F32)
                return jnp.dot(jnp.exp2(scores).astype(BF16), value, preferred_element_type=F32)

            one = head(jnp.where(query_low, query_pair, none), value_one)
            two = head(jnp.where(query_low, none, query_pair), value_two)
            low = lax.broadcasted_iota(jnp.int32, one.shape, 1) < 64
            top = jnp.where(low, one, two)
            total = pltpu.roll(jnp.where(low, two, one), 64, 1)
            attended[rows, cols] = (top / total).astype(BF16)

    @pl.loop(0, HEADS // 4)
    def _(pair):
        attend(pair)

    for quarter in range(4):
        stage_four(O, quarter)

    @pl.loop(HEADS // 4, HEADS // 2)
    def _(pair):
        attend(pair)

    finish(O)
    for chunk in range(2):
        rows = slice(chunk * 256, chunk * 256 + 256)
        for half in range(2):
            update[rows, half * SLAB:(half + 1) * SLAB] = jnp.dot(
                attended[rows, :], full[2 * O + half], preferred_element_type=F32).astype(BF16)
    for copy in sent:
        copy.wait_send()
    for part in (Q, K, V, O):
        all_pieces(part, plane_send)
        all_pieces(part, pair_send)


def shards(fields, cell_index, interp_weight, w_in, ln_gain, w_qkv, w_out):
    hbm = pl.BlockSpec(memory_space=pltpu.MemorySpace.HBM)
    dma = pltpu.SemaphoreType.DMA
    vmem = pltpu.VMEM
    latent, update = pl.pallas_call(
        everything,
        out_shape=(jax.ShapeDtypeStruct((NODE, 1024), BF16),) * 2,
        in_specs=[hbm] * 7,
        out_specs=(pl.BlockSpec(memory_space=pltpu.VMEM),) * 2,
        scratch_shapes=[
            pltpu.SMEM((BLK, LANES), jnp.int32),
            vmem((BLK, 16, LANES), BF16),
            vmem((CH, 1024), BF16),
            vmem((1, 1024), F32),
            vmem((CH, REACH), BF16),
            vmem((REACH, LANES), F32),
            vmem((BLK * LANES, LANES), F32),
            vmem((2 * NODE, LANES), BF16),
            vmem((8, 1024, SLAB), BF16),
            vmem((LANES, 1024), BF16),
            vmem((2 * NODE, 1024), BF16),
            vmem((2 * NODE, 1024), F32),
            vmem((NODE, 1024), BF16),
            vmem((2 * NODE, 1024), BF16),
            vmem((2 * NODE, 1024), BF16),
            vmem((NODE, 1024), BF16),
            dma((8,)), dma((8,)), dma((2,)), dma((2,)), dma((2,)), dma((2,)),
            dma((4,)), dma((80,)), dma((4,)), dma((4,)),
        ],
        compiler_params=pltpu.CompilerParams(
            collective_id=0, has_side_effects=True, vmem_limit_bytes=40 * 1024 * 1024),
        name="everything",
    )(*(pltpu.with_memory_space_constraint(array, pltpu.MemorySpace.HBM) for array in (
        fields[0], cell_index, interp_weight, w_in, ln_gain[None], w_qkv, w_out)))
    return (latent[None], update[None])


def solution(mesh):
    placed = (
        P("dp", None, "space"),
        P("space", None),
        P("space", None, None),
        P(),
        P(),
        P("dp", None),
        P("dp", None),
    )
    return jax.shard_map(
        shards,
        mesh=mesh,
        in_specs=placed,
        out_specs=(P("dp", "space", None), P("dp", "space", None)),
        check_vma=False,
    )
```

```python
import math

import jax
import jax.numpy as jnp
from jax import lax
from jax.experimental import pallas as pl
from jax.experimental.pallas import tpu as pltpu
from jax.sharding import PartitionSpec as P

HEADS = 16
CH = 100
HALO_C = 1024
HALO_N = 256
NODE = 512
BLK = 32
CELL = 4096
REACH = CELL + 2 * HALO_C
LANES = 128
SHARD = 64
SLAB = 512
WIDE = 256
MESH = pl.DeviceIdType.MESH
F32, BF16 = jnp.float32, jnp.bfloat16
Q, K, V, O = 0, 1, 2, 3
FIRST = {Q: "x", K: "y", V: "y", O: "y"}
ORDER = (K, Q, V)
RELATIVE = (0, -1, 1, 2)


def everything(
    fields, index_hbm, weight_hbm, w_in_hbm, gain_hbm, w_qkv, w_out,
    latent, update,
    index, weight, w_in, gain, ext, ext_t, picked, enc, full,
    w_pad, normed, raw, queries, keys, values, attended,
    local_sem, own_sem, cell_send, cell_recv, enc_send, enc_recv,
    plane_send, plane_recv, pair_send, pair_recv,
):
    dp = lax.axis_index("dp")
    sp = lax.axis_index("space")
    x, y = dp % 4, dp // 4
    core, side, z = sp % 2, (sp // 2) % 2, sp // 4

    def at(new_y, new_x, new_z, new_side, new_core):
        return (new_y * 4 + new_x, new_z * 4 + new_side * 2 + new_core)

    up_side = (side + (y + 1) // 4) % 2
    down_side = (side + 1 - (y + 3) // 4) % 2
    step_to = {
        ("x", 1): at(y, (x + 1) % 4, z, side, core),
        ("x", -1): at(y, (x + 3) % 4, z, side, core),
        ("y", 1): at((y + 1) % 4, x, z, up_side, core),
        ("y", -1): at((y + 3) % 4, x, z, down_side, core),
    }
    partner = at(y, x, z, side, 1 - core)
    left = (dp, (sp + 31) % 32)
    right = (dp, (sp + 1) % 32)
    far = (dp, (sp + 31 + 2 * core) % 32)

    own_cells = pltpu.make_async_copy(fields, ext.at[:, pl.ds(HALO_C, CELL)], local_sem.at[0])
    own_cells.start()
    small = [
        pltpu.make_async_copy(source, place, local_sem.at[1 + i])
        for i, (source, place) in enumerate(
            ((index_hbm, index), (weight_hbm, weight), (w_in_hbm, w_in), (gain_hbm, gain)))
    ]
    for copy in small:
        copy.start()

    def shard(part, half):
        if part == O:
            return w_out.at[:, pl.ds(pl.multiple_of(half * SLAB, SLAB), SLAB)]
        return w_qkv.at[:, pl.ds(pl.multiple_of(part * 1024 + half * SLAB, SLAB), SLAB)]

    own_rows = {}
    for part in (K, Q, V, O):
        for half in range(2):
            own_rows[part, half] = pltpu.make_async_copy(
                shard(part, half),
                full.at[2 * part + half, pl.ds(pl.multiple_of(dp * SHARD, SHARD), SHARD)],
                own_sem.at[2 * part + half])
            own_rows[part, half].start()

    barrier = pltpu.get_barrier_semaphore()
    for other in list(step_to.values()) + [partner, far]:
        pl.semaphore_signal(barrier, inc=1, device_id=other, device_id_type=MESH)
    pl.semaphore_wait(barrier, 6)

    sent = []

    def remote(src, dst, s_sem, r_sem, target, grouped=False):
        copy = pltpu.make_async_remote_copy(
            src_ref=src, dst_ref=dst, send_sem=s_sem, recv_sem=r_sem,
            device_id=target, device_id_type=MESH,
        )
        copy.start()
        if not grouped:
            sent.append(copy)
        return copy

    def place(part, first, second, begin=0, size=SHARD):
        if FIRST[part] == "x":
            piece_y, piece_x = (y + 4 + second) % 4, (x + 4 + first) % 4
        else:
            piece_y, piece_x = (y + 4 + first) % 4, (x + 4 + second) % 4
        start = pl.multiple_of((piece_y * 4 + piece_x) * SHARD + begin, 32)
        return full.at[2 * part + core, pl.ds(start, size)]

    plane = {}

    def move(part, first, second, axis, direction, number, begin=0, size=SHARD):
        target = place(part, first, second, begin, size)
        source = target
        if first == 0 and second == 0:
            source = shard(part, core)
        plane[part, number] = remote(
            source, target, plane_send.at[part], plane_recv.at[part * 20 + number],
            step_to[axis, direction], grouped=True)

    def second_axis(part):
        return "y" if FIRST[part] == "x" else "x"

    def hand_on(part, first, second, unit):
        here = place(part, first, second)
        remote(here, here, pair_send.at[part], pair_recv.at[part], partner, grouped=True)

    def all_pieces(part, sem):
        rows = full.at[2 * part, pl.ds(0, 15 * SHARD)]
        pltpu.make_async_copy(rows, rows, sem.at[part]).wait()

    def outward(part, first_at):
        for kind, direction in ((0, 1), (1, -1)):
            move(part, RELATIVE[first_at], 0, second_axis(part), direction, 4 + 4 * first_at + kind)

    def begin(parts):
        for part in parts:
            move(part, 0, 0, FIRST[part], 1, 0)
            move(part, 0, 0, FIRST[part], -1, 1)
        for part in parts:
            outward(part, 0)

    for part in (K, V):
        move(part, 0, 0, FIRST[part], 1, 0)
        move(part, 0, 0, FIRST[part], -1, 1)
    cells_right = remote(
        fields.at[:, pl.ds(CELL - HALO_C, HALO_C)], ext.at[:, pl.ds(0, HALO_C)],
        cell_send.at[0], cell_recv.at[0], right)
    cells_left = remote(
        fields.at[:, pl.ds(0, HALO_C)], ext.at[:, pl.ds(HALO_C + CELL, HALO_C)],
        cell_send.at[1], cell_recv.at[1], left)
    outward(K, 0)
    outward(V, 0)
    move(Q, 0, 0, FIRST[Q], 1, 0)
    move(Q, 0, 0, FIRST[Q], -1, 1)

    def stage_one(part):
        for kind, relative, direction, begin in ((0, -1, 1, 0), (1, 1, -1, 32)):
            plane[part, kind].wait_recv()
            move(part, relative, 0, FIRST[part], direction, 2 + kind, begin, 32)
            outward(part, 1 + kind)
            hand_on(part, relative, 0, kind)

    def stage_two(part):
        plane[part, 2].wait_recv()
        plane[part, 3].wait_recv()
        outward(part, 3)
        hand_on(part, 2, 0, 2)

    def stage_three(part, first_at):
        for kind, relative, direction, begin in ((0, -1, 1, 0), (1, 1, -1, 32)):
            number = 4 + 4 * first_at
            plane[part, number + kind].wait_recv()
            move(part, RELATIVE[first_at], relative, second_axis(part), direction,
                 number + 2 + kind, begin, 32)
            hand_on(part, RELATIVE[first_at], relative, 3 + 3 * first_at + kind)

    def stage_four(part, first_at):
        number = 4 + 4 * first_at
        plane[part, number + 2].wait_recv()
        plane[part, number + 3].wait_recv()
        hand_on(part, RELATIVE[first_at], 2, 3 + 3 * first_at + 2)

    def finish(part):
        for half in range(2):
            own_rows[part, half].wait()
        all_pieces(part, pair_recv)

    def turn(start, count):
        @pl.loop(0, count // 4)
        def _(i):
            for k in range(4):
                at_cell = pl.multiple_of(start + i * (4 * LANES) + k * LANES, LANES)
                ext_t[pl.ds(at_cell, LANES), 0:CH] = ext[:, pl.ds(at_cell, LANES)].astype(F32).T

    def encode(first_block, count):
        @pl.loop(first_block, first_block + count)
        def _(b):
            base = pl.multiple_of(b * LANES, LANES)
            for j in range(LANES):
                picked[pl.ds(base + j, 1), :] = ext_t[pl.ds(index[b, j], 1), :]
        for b in range(first_block, first_block + count):
            rows = picked[b * LANES:(b + 1) * LANES, :].astype(BF16)
            mixed = jnp.dot(weight[b], rows, preferred_element_type=F32)
            lane = lax.broadcasted_iota(jnp.int32, mixed.shape, 1)
            enc[b * 16:(b + 1) * 16, :] = jnp.where(lane < CH, mixed, 0.0).astype(BF16)

    def embed(chunk, keep):
        rows = slice(chunk * 128, chunk * 128 + 128)
        embedded = jnp.dot(enc[rows, :], w_pad[...], preferred_element_type=F32)
        if keep:
            latent[rows, :] = embedded.astype(BF16)
        average = jnp.mean(embedded, axis=1, keepdims=True)
        centered = embedded - average
        spread = jnp.mean(centered * centered, axis=1, keepdims=True)
        normed[rows, :] = (centered * lax.rsqrt(spread + 1e-05) * gain[...]).astype(BF16)

    row_head = lax.broadcasted_iota(jnp.int32, (WIDE, WIDE), 0) // 64
    col_head = lax.broadcasted_iota(jnp.int32, (WIDE, WIDE), 1) // 64
    same_head = jnp.where(row_head == col_head, 1.0, 0.0).astype(BF16)

    def unit_rows(projected, factor):
        squares = (projected * projected).astype(BF16)
        total = jnp.dot(squares, same_head, preferred_element_type=F32)
        return (projected * (lax.rsqrt(total * (1.0 / 64) + 1e-06) * factor)).astype(BF16)

    def project(part):
        @pl.loop(0, 4)
        def _(group):
            cols = pl.ds(pl.multiple_of(group * WIDE, WIDE), WIDE)
            block = full[2 * part + group // 2, :, pl.ds(pl.multiple_of((group % 2) * WIDE, WIDE), WIDE)]
            for chunk in range(2 if part == Q else 4):
                rows = slice(chunk * 256, chunk * 256 + 256)
                projected = jnp.dot(normed[rows, :], block, preferred_element_type=F32)
                if part == V:
                    values[rows, cols] = projected.astype(BF16)
                else:
                    raw[rows, cols] = projected
        if part == V:
            return

        @pl.loop(0, 4)
        def _(group):
            cols = pl.ds(pl.multiple_of(group * WIDE, WIDE), WIDE)
            for chunk in range(2 if part == Q else 4):
                rows = slice(chunk * 256, chunk * 256 + 256)
                if part == Q:
                    queries[rows, cols] = unit_rows(raw[rows, cols], math.log2(math.e) / 8)
                else:
                    keys[rows, cols] = unit_rows(raw[rows, cols], 1.0)

    own_cells.wait()
    for copy in small:
        copy.wait()
    w_pad[...] = jnp.zeros_like(w_pad)
    w_pad[0:CH, :] = w_in[...]
    turn(HALO_C, CELL // LANES)
    stage_one(K)
    stage_one(V)
    stage_three(K, 0)
    stage_three(V, 0)
    cells_right.wait_recv()
    turn(0, HALO_C // LANES)
    cells_left.wait_recv()
    turn(HALO_C + CELL, HALO_C // LANES)
    encode(0, 8)
    stage_two(K)
    stage_three(K, 1)
    encode(8, 8)
    enc_left = remote(
        enc.at[pl.ds(0, HALO_N)], enc.at[pl.ds(NODE + HALO_N, HALO_N)],
        enc_send.at[0], enc_recv.at[0], left)
    stage_two(V)
    stage_three(V, 1)
    encode(16, 8)
    stage_three(K, 2)
    stage_three(V, 2)
    encode(24, 8)
    enc_right = remote(
        enc.at[pl.ds(NODE - HALO_N, HALO_N)], enc.at[pl.ds(NODE, HALO_N)],
        enc_send.at[1], enc_recv.at[1], right)
    outward(Q, 0)
    stage_one(Q)
    embed(0, True)
    embed(1, True)
    stage_three(K, 3)
    stage_three(V, 3)
    embed(2, True)
    stage_two(Q)
    embed(3, True)
    for quarter in range(4):
        stage_four(K, quarter)
    enc_left.wait_recv()
    enc_right.wait_recv()
    for quarter in range(4):
        embed(4 + quarter, False)
        stage_four(V, quarter)
    for quarter in range(4):
        stage_three(Q, quarter)
    begin((O,))
    finish(K)
    project(K)
    for quarter in range(4):
        stage_four(Q, quarter)
    stage_one(O)
    finish(V)
    project(V)
    stage_two(O)
    finish(Q)
    project(Q)
    for quarter in range(4):
        stage_three(O, quarter)

    def attend(pair):
        cols = pl.ds(pl.multiple_of(pair * LANES, LANES), LANES)
        key_pair = keys[:, cols]
        value_pair = values[:, cols]
        value_low = lax.broadcasted_iota(jnp.int32, value_pair.shape, 1) < 64
        ones = jnp.ones_like(value_pair)
        value_one = jnp.where(value_low, value_pair, ones)
        value_two = jnp.where(value_low, ones, value_pair)
        for chunk in range(2):
            rows = slice(chunk * 256, chunk * 256 + 256)
            query_pair = queries[rows, cols]
            query_low = lax.broadcasted_iota(jnp.int32, query_pair.shape, 1) < 64
            none = jnp.zeros_like(query_pair)

            def head(query, value):
                scores = lax.dot_general(
                    query, key_pair, (((1,), (1,)), ((), ())), preferred_element_type=F32)
                return jnp.dot(jnp.exp2(scores).astype(BF16), value, preferred_element_type=F32)

            one = head(jnp.where(query_low, query_pair, none), value_one)
            two = head(jnp.where(query_low, none, query_pair), value_two)
            low = lax.broadcasted_iota(jnp.int32, one.shape, 1) < 64
            top = jnp.where(low, one, two)
            total = pltpu.roll(jnp.where(low, two, one), 64, 1)
            attended[rows, cols] = (top / total).astype(BF16)

    @pl.loop(0, HEADS // 4)
    def _(pair):
        attend(pair)

    for quarter in range(4):
        stage_four(O, quarter)

    @pl.loop(HEADS // 4, HEADS // 2)
    def _(pair):
        attend(pair)

    finish(O)
    for chunk in range(2):
        rows = slice(chunk * 256, chunk * 256 + 256)
        for half in range(2):
            update[rows, half * SLAB:(half + 1) * SLAB] = jnp.dot(
                attended[rows, :], full[2 * O + half], preferred_element_type=F32).astype(BF16)
    for copy in sent:
        copy.wait_send()
    for part in (Q, K, V, O):
        all_pieces(part, plane_send)
        all_pieces(part, pair_send)


def shards(fields, cell_index, interp_weight, w_in, ln_gain, w_qkv, w_out):
    hbm = pl.BlockSpec(memory_space=pltpu.MemorySpace.HBM)
    dma = pltpu.SemaphoreType.DMA
    vmem = pltpu.VMEM
    latent, update = pl.pallas_call(
        everything,
        out_shape=(jax.ShapeDtypeStruct((NODE, 1024), BF16),) * 2,
        in_specs=[hbm] * 7,
        out_specs=(pl.BlockSpec(memory_space=pltpu.VMEM),) * 2,
        scratch_shapes=[
            pltpu.SMEM((BLK, LANES), jnp.int32),
            vmem((BLK, 16, LANES), BF16),
            vmem((CH, 1024), BF16),
            vmem((1, 1024), F32),
            vmem((CH, REACH), BF16),
            vmem((REACH, LANES), F32),
            vmem((BLK * LANES, LANES), F32),
            vmem((2 * NODE, LANES), BF16),
            vmem((8, 1024, SLAB), BF16),
            vmem((LANES, 1024), BF16),
            vmem((2 * NODE, 1024), BF16),
            vmem((2 * NODE, 1024), F32),
            vmem((NODE, 1024), BF16),
            vmem((2 * NODE, 1024), BF16),
            vmem((2 * NODE, 1024), BF16),
            vmem((NODE, 1024), BF16),
            dma((8,)), dma((8,)), dma((2,)), dma((2,)), dma((2,)), dma((2,)),
            dma((4,)), dma((80,)), dma((4,)), dma((4,)),
        ],
        compiler_params=pltpu.CompilerParams(
            collective_id=0, has_side_effects=True, vmem_limit_bytes=40 * 1024 * 1024),
        name="everything",
    )(*(pltpu.with_memory_space_constraint(array, pltpu.MemorySpace.HBM) for array in (
        fields[0], cell_index, interp_weight, w_in, ln_gain[None], w_qkv, w_out)))
    return (latent[None], update[None])


def solution(mesh):
    placed = (
        P("dp", None, "space"),
        P("space", None),
        P("space", None, None),
        P(),
        P(),
        P("dp", None),
        P("dp", None),
    )
    return jax.shard_map(
        shards,
        mesh=mesh,
        in_specs=placed,
        out_specs=(P("dp", "space", None), P("dp", "space", None)),
        check_vma=False,
    )
```
